32 devices in a mesh: front: 4 (over y, core), blk: 8 (over z, x).
Axes of the slice: x: 2, y: 2, z: 4, core: 2. Of those that a mesh axis runs over, the one named last changes fastest.
Arguments:
- front: float32 [4, 1024, 1024], P('front', 'blk'), parts along dimension 0, may hold values from -8 to 40, as said below
- child: float32 [4, 512, 512], P('front', 'blk'), parts along dimension 0, may hold values from -1 to 4, as said below
- index_map: int32 [2048], P('front'), parts along dimension 0, may hold values from 0 to 1023, as said below
Outputs:
- factored: float32 [4, 1024, 1024], P('front', 'blk'), parts along dimension 0
The draws below stay inside these ranges and needn't reach their ends.
There are 4 independent parts, one for each index of `front`. The reference program is written for one: setup_inputs(seed, part) draws one part's arguments, and reference() takes and returns one part's arrays. A program takes and returns all parts, laid end to end along the dimension named above; each array names one. Nothing has to cross between parts.
Inputs may be any that keep to these rules, and one draw needn't show every extreme that they name: front is symmetric and positive definite. child is symmetric and positive semidefinite. `index_map`: tile t of the child (indices t * 64 to t * 64 + 63, with t = k * 8 + e and e < 8) maps in increasing order onto 64 different indices of the front's block column b = k * 8 + ((e + h) mod 8), where h is half of 8, that is onto indices b * 128 to b * 128 + 127; no two child indices share a front index.
All inputs are finite; a program needn't handle non-finite values.
Results may differ from the reference program's by a relative error of at most 0.0034.
Values may be sent and summed in bfloat16 or wider, within the bound.
No kernel may reach another device: no remote copies, remote signals or barrier semaphores. Data moves between devices by JAX's collectives and lax.ppermute only.
A program may use at most 128 MiB of HBM per device.

```python
import math
import jax
import jax.numpy as jnp
from jax import lax

PANEL_WIDTH = 512
BLOCK_WIDTH = 128
COL_BLOCKS = 1
FRONT_ORDER = 1024
CHILD_ORDER = 512
TILE_WIDTH = 64
N_BLK = 8


def symmetric_noise(subkey, matrix_order, spread):
    normal_draw = jax.random.normal(subkey, (matrix_order, matrix_order), jnp.float32)
    return (normal_draw + normal_draw.T) * (spread / math.sqrt(2.0))


def draw_front(key, part):
    subkeys = jax.random.split(jax.random.fold_in(key, 101), 2)
    coupling_rank = 2 * PANEL_WIDTH
    coupling = jax.random.normal(subkeys[0], (FRONT_ORDER, coupling_rank), jnp.float32)
    coupling = coupling * (2.0 / math.sqrt(coupling_rank))
    matrix = jnp.dot(coupling, coupling.T, precision=lax.Precision.HIGHEST)
    matrix = matrix + symmetric_noise(subkeys[1], FRONT_ORDER, 0.25 / math.sqrt(FRONT_ORDER))
    matrix = matrix + jnp.eye(FRONT_ORDER, dtype=jnp.float32)
    return matrix.reshape(COL_BLOCKS, N_BLK * BLOCK_WIDTH, FRONT_ORDER)


def draw_child(key, part):
    subkeys = jax.random.split(jax.random.fold_in(key, 202), 2)
    levels = jax.random.uniform(subkeys[0], (CHILD_ORDER,), jnp.float32, 1.5, 3.0)
    matrix = jnp.diag(levels) + symmetric_noise(subkeys[1], CHILD_ORDER, 0.5 / math.sqrt(CHILD_ORDER))
    return matrix.reshape(COL_BLOCKS, N_BLK * TILE_WIDTH, CHILD_ORDER)


def pick_subset(subkey):
    return jax.random.permutation(subkey, BLOCK_WIDTH)[:TILE_WIDTH]


def draw_index_map(key, part):
    tile_count = FRONT_ORDER // BLOCK_WIDTH
    subkeys = jax.random.split(jax.random.fold_in(key, 303), tile_count)
    chosen = jnp.sort(jax.vmap(pick_subset)(subkeys).astype(jnp.int32), axis=1)
    tile_ids = jnp.arange(tile_count, dtype=jnp.int32)
    target = tile_ids // N_BLK * N_BLK + (tile_ids % N_BLK + N_BLK // 2) % N_BLK
    return (target[:, None] * BLOCK_WIDTH + chosen).reshape(-1).astype(jnp.int32)


def setup_inputs(seed: int = 0, part: int = 0) -> dict:
    streams_of = jax.random.split(jax.random.key(seed), 4)
    own_keys = jax.random.split(jax.random.fold_in(streams_of[3], part), 4)
    front = draw_front(jax.random.fold_in(jax.random.fold_in(streams_of[3], part), 71), part)
    child = draw_child(jax.random.fold_in(jax.random.fold_in(streams_of[3], part), 71), part)
    index_map = draw_index_map(jax.random.fold_in(jax.random.fold_in(streams_of[3], part), 71), part)
    return dict(front=front, child=child, index_map=index_map)


def factor_rows(matrix, row_start):
    diag_factor = jnp.linalg.cholesky(matrix[row_start:row_start + PANEL_WIDTH, row_start:row_start + PANEL_WIDTH])
    panel_part = matrix[:, row_start:row_start + PANEL_WIDTH]
    solved = lax.linalg.triangular_solve(diag_factor, panel_part, left_side=False, lower=True, transpose_a=True)
    offsets = jnp.arange(FRONT_ORDER, dtype=jnp.int32) - row_start
    diag_rows = jnp.take(diag_factor, jnp.clip(offsets, 0, PANEL_WIDTH - 1), axis=0)
    inside = (offsets >= 0) & (offsets < PANEL_WIDTH)
    before = offsets < 0
    return jnp.where(inside[:, None], diag_rows, jnp.where(before[:, None], jnp.zeros((), solved.dtype), solved))

def reference(front, child, index_map):
    matrix = front.reshape(FRONT_ORDER, FRONT_ORDER)
    contribution = child.reshape(CHILD_ORDER, CHILD_ORDER)
    matrix = matrix.at[index_map[:, None], index_map[None, :]].add(contribution)
    for row_start in (0, PANEL_WIDTH):
        lowered = factor_rows(matrix, row_start).astype(jnp.bfloat16)
        cutoff = row_start + PANEL_WIDTH
        remaining = matrix[cutoff:] - jnp.dot(lowered[cutoff:].astype(jnp.float32), lowered.T.astype(jnp.float32), preferred_element_type=jnp.float32)
        matrix = jnp.concatenate([matrix[:row_start], lowered.T.astype(matrix.dtype), remaining], axis=0)
    positions = jnp.arange(FRONT_ORDER, dtype=jnp.int32)
    cleared = (positions[:, None] >= 2 * PANEL_WIDTH) & (positions[None, :] < 2 * PANEL_WIDTH)
    matrix = jnp.where(cleared, jnp.zeros((), matrix.dtype), matrix)
    return matrix.reshape(COL_BLOCKS, N_BLK * BLOCK_WIDTH, FRONT_ORDER)
```

```python
import jax
import jax.numpy as jnp
from jax import lax
from jax.experimental import pallas as pl
from jax.experimental.pallas import tpu as pltpu
from jax.sharding import PartitionSpec as P

PANEL_WIDTH = 512
BLOCK_WIDTH = 128
COL_BLOCKS = 1
TILE_WIDTH = 64


HIGHEST = lax.Precision.HIGHEST


F32 = jnp.float32
BF16 = jnp.bfloat16
LANES = 128
SUBS = 8
WIDTH = 2
GROUP = 4

def lane_copy(tile, lane):
    return jnp.broadcast_to(tile[:, lane:lane+1], tile.shape)

def row_copy(tile, row):
    return jnp.broadcast_to(tile[row:row+1, :], tile.shape)

def tree_sum(terms):
    while len(terms) > 1:
        terms = [a + b for a, b in zip(terms[::2], terms[1::2])] + ([terms[-1]] if len(terms) % 2 else [])
    return terms[0]

def halves(x):
    high = x.astype(BF16)
    return high, (x - high.astype(F32)).astype(BF16)

def dot3(a, b, dims=(((1,), (0,)), ((), ()))):
    ah, al = halves(a)
    bh, bl = halves(b)
    mm = lambda x, y: lax.dot_general(x, y, dims, preferred_element_type=F32)
    return mm(ah, bh) + (mm(ah, bl) + mm(al, bh))

def eliminate(tiles, start_lane, zero):
    count = len(tiles)
    tiles = list(tiles)
    shape = (SUBS, LANES)
    lane = lax.broadcasted_iota(jnp.int32, shape, 1)
    sub = lax.broadcasted_iota(jnp.int32, shape, 0)
    at_row = [sub == k for k in range(SUBS)]
    uppers, inverses = [], []
    for head in range(0, count, WIDTH):
        own = range(WIDTH)
        span = WIDTH * SUBS
        first = start_lane + head * SUBS
        inside = (lane >= first) & (lane < first + span)
        cols = [[None] * span for _ in own]
        for m in range(span):
            for t in own:
                cols[t][m] = lane_copy(tiles[head + t], first + m) + zero
        later = {}
        for m in range(span):
            for i in range(head + WIDTH, count):
                later[i, m] = lane_copy(tiles[i], first + m)
        plain = [tiles[head + t] for t in own]
        joined = [
            jnp.where(inside, jnp.where(lane - (first + t * SUBS) == sub, 1.0, 0.0), plain[t]) for t in own
        ]
        upper = [jnp.zeros(shape, F32) for _ in own]
        inverse = [jnp.zeros(shape, F32) for _ in own]
        for k in range(span):
            at, r = divmod(k, SUBS)
            root = lax.rsqrt(row_copy(cols[at][k], r))
            inv = root * root
            weight = [jnp.where(at_row[r], -1.0, cols[t][k]) if t == at else cols[t][k] for t in own]
            for m in range(k + 1, span):
                pivot = row_copy(cols[at][m], r)
                for t in own:
                    kept = jnp.where(at_row[r], 0.0, cols[t][m]) if t == at else cols[t][m]
                    if m == k + 1:
                        cols[t][m] = kept - (weight[t] * pivot) * inv
                    else:
                        if t == 0:
                            scaled = pivot * inv
                        cols[t][m] = kept - weight[t] * scaled
            pivot = row_copy(plain[at], r)
            upper[at] = jnp.where(at_row[r], pivot * root, upper[at])
            scaled = pivot * inv
            for t in range(at, WIDTH):
                plain[t] = plain[t] - weight[t] * scaled
            pivot = row_copy(joined[at], r)
            inverse[at] = jnp.where(at_row[r], pivot * root, inverse[at])
            scaled = pivot * inv
            for t in own:
                kept = jnp.where(at_row[r], 0.0, joined[t]) if t == at else joined[t]
                joined[t] = kept - weight[t] * scaled
        for t in own:
            diag = first + t * SUBS + sub
            uppers.append(jnp.where(lane >= diag, upper[t], 0.0))
            inverses.append(jnp.where(lane <= diag, inverse[t], 0.0))
        rows = [row_copy(joined[k // SUBS], k % SUBS) for k in range(span)]
        for i in range(head + WIDTH, count):
            update = tree_sum([later[i, k] * rows[k] for k in range(span)])
            tiles[i] = jnp.where(inside, 0.0, tiles[i]) - update
    return uppers, inverses

def factor_tiles(tiles, zero):
    tiles = list(tiles)
    lane = lax.broadcasted_iota(jnp.int32, (SUBS, LANES), 1)
    uppers, inverses = [], []
    for g in range(0, len(tiles), GROUP):
        up, inv = eliminate(tiles[g:g+GROUP], g*SUBS, zero)
        uppers += up; inverses += inv
        done = (g + GROUP) * SUBS
        rest = len(tiles) - g - GROUP
        if rest:
            z = jnp.concatenate([jnp.where(lane < done, a, b) for a, b in zip(inv, up)], axis=0)
            left = z.T[done:, :]
            upd = dot3(left, z)
            for t in range(rest):
                i = g + GROUP + t
                tiles[i] = jnp.where((lane >= g*SUBS) & (lane < done), 0.0, tiles[i]) - upd[8*t:8*t+8, :]
    return uppers, inverses


def spread(children, row_hot, col_hot, add):
    pair = 2 * TILE_WIDTH
    pairs = children.shape[0] // pair
    parts = []
    left = children
    for _ in range(3):
        parts.append(left.astype(BF16))
        left = left - parts[-1].astype(F32)
    for p in range(pairs):
        down = [
            jnp.dot(row_hot[:, p * pair : (p + 1) * pair], part[p * pair : (p + 1) * pair, :], preferred_element_type=F32).astype(BF16)
            for part in parts
        ]
        for q in range(pairs):
            total = sum(
                jnp.dot(d[:, q * pair : (q + 1) * pair], col_hot[q * pair : (q + 1) * pair, :], preferred_element_type=F32)
                for d in down
            )
            add(p, q, total)


def load_square(me, slabs, tiles, row_hot, col_hot, kids, square, lane_start):
    count = len(slabs)
    for m in range(count):
        owner = jnp.bitwise_xor(me, m)
        for j in range(count):
            square[j, pl.ds(pl.multiple_of(owner * BLOCK_WIDTH, BLOCK_WIDTH), BLOCK_WIDTH), :] = slabs[m][
                :, j * BLOCK_WIDTH : (j + 1) * BLOCK_WIDTH
            ]
        kids[pl.ds(pl.multiple_of(owner * TILE_WIDTH, TILE_WIDTH), TILE_WIDTH), :] = tiles[m][
            :, lane_start : lane_start + count * TILE_WIDTH
        ]

    def add(p, q, total):
        rows = slice(p * 2 * BLOCK_WIDTH, (p + 1) * 2 * BLOCK_WIDTH)
        for half in range(2):
            square[2 * q + half, rows, :] += total[:, half * BLOCK_WIDTH : (half + 1) * BLOCK_WIDTH]

    spread(kids[...], row_hot[...], col_hot[...], add)


def block_rows(b):
    return pl.ds(pl.multiple_of(b * BLOCK_WIDTH, BLOCK_WIDTH), BLOCK_WIDTH)


def factor_panel(square, inverse, zero):
    count = square.shape[0]

    def body(b, _):
        rows = block_rows(b)
        base = pl.multiple_of(b * BLOCK_WIDTH, BLOCK_WIDTH)
        tiles = [square[b, pl.ds(base + SUBS * t, SUBS), :] for t in range(BLOCK_WIDTH // SUBS)]
        uppers, inverses = factor_tiles(tiles, zero)
        for t in range(BLOCK_WIDTH // SUBS):
            square[b, pl.ds(base + SUBS * t, SUBS), :] = uppers[t]
            inverse[pl.ds(base + SUBS * t, SUBS), :] = inverses[t]
        own_inverse = inverse[rows, :]

        def solve(j, _):
            square[j, rows, :] = dot3(own_inverse, square[j, rows, :])
            return 0

        lax.fori_loop(b + 1, count, solve, 0)

        def update(i, _):
            left = square[i, rows, :].T

            def inner(j, _):
                square[j, block_rows(i), :] -= dot3(left, square[j, rows, :])
                return 0

            return lax.fori_loop(i, count, inner, 0)

        return lax.fori_loop(b + 1, count, update, 0)

    lax.fori_loop(0, count, body, 0)


def first_kernel(me, *refs):
    count = PANEL_WIDTH // BLOCK_WIDTH
    slabs, tiles = refs[:count], refs[count : 2 * count]
    row_hot, col_hot, upper, inverse, kids = refs[2 * count :]
    load_square(me[0], slabs, tiles, row_hot, col_hot, kids, upper, 0)
    factor_panel(upper, inverse, slabs[0][:SUBS, :LANES] * 0.0)


def second_kernel(me, *refs):
    count = PANEL_WIDTH // BLOCK_WIDTH
    sides, fars, tiles = refs[:count], refs[count : 2 * count], refs[2 * count : 3 * count]
    upper, inverse, row_hot, far_row_hot, col_hot, mine, send, side, square, own_inverse, kids = refs[3 * count :]
    load_square(me[0], sides, tiles, row_hot, col_hot, kids, side, 0)
    load_square(me[0], fars, tiles, far_row_hot, col_hot, kids, square, count * TILE_WIDTH)
    for b in range(count):
        rows = slice(b * BLOCK_WIDTH, (b + 1) * BLOCK_WIDTH)
        for j in range(count):
            side[j, rows, :] = dot3(inverse[rows, :], side[j, rows, :])
        for i in range(b + 1, count):
            left = upper[i, rows, :].T
            for j in range(count):
                side[j, i * BLOCK_WIDTH : (i + 1) * BLOCK_WIDTH, :] -= dot3(left, side[j, rows, :])
    rounded = [side[j].astype(BF16) for j in range(count)]
    for i in range(count):
        left = rounded[i].T
        for j in range(i, count):
            square[j, i * BLOCK_WIDTH : (i + 1) * BLOCK_WIDTH, :] -= jnp.dot(left, rounded[j], preferred_element_type=F32)
    factor_panel(square, own_inverse, sides[0][:SUBS, :LANES] * 0.0)
    rows = block_rows(me[0])
    for j in range(count):
        lanes = slice(j * BLOCK_WIDTH, (j + 1) * BLOCK_WIDTH)
        mine[:, lanes] = jnp.where(j >= me[0], upper[j, rows, :], 0.0).astype(BF16).astype(F32)
        mine[:, PANEL_WIDTH + j * BLOCK_WIDTH : PANEL_WIDTH + (j + 1) * BLOCK_WIDTH] = (
            side[j, rows, :].astype(BF16).astype(F32)
        )
        send[:, lanes] = jnp.where(j >= me[0], square[j, rows, :], 0.0).astype(BF16)


def two_panels(front, child, index_map):
    cycle_size = lax.axis_size("blk")
    my_index = lax.axis_index("blk")
    count = PANEL_WIDTH // BLOCK_WIDTH
    span = count * TILE_WIDTH
    me = my_index % count
    half = my_index // count

    def swap(shard, by):
        return lax.ppermute(shard, "blk", [(i, i ^ by) for i in range(cycle_size)])

    def part(array, which, width):
        return lax.dynamic_slice_in_dim(array, which * width, width, array.ndim - 1)

    def hot(which):
        places = part(index_map, which, span) % BLOCK_WIDTH + jnp.arange(span, dtype=jnp.int32) // TILE_WIDTH % 2 * BLOCK_WIDTH
        wide = jnp.arange(2 * BLOCK_WIDTH, dtype=jnp.int32)
        return (wide[:, None] == places).astype(BF16), (places[:, None] == wide).astype(BF16)

    slab, kids = front[0], child[0]
    row_hot, col_hot = hot(1 - half)
    far_row_hot, far_col_hot = hot(half)
    diag = part(slab, half, PANEL_WIDTH)
    side = part(slab, 1 - half, PANEL_WIDTH)
    arrived = swap(kids, count)
    diags = [diag] + [swap(diag, m) for m in range(1, count)]
    diag_kids = part(arrived, 1 - half, span)
    diag_tiles = [diag_kids] + [swap(diag_kids, m) for m in range(1, count)]
    far = swap(diag, count)
    sides = [side] + [swap(side, m) for m in range(1, count)]
    later = jnp.concatenate([part(arrived, half, span), part(kids, half, span)], axis=1)
    tiles = [later] + [swap(later, m) for m in range(1, count)]
    fars = [far] + [swap(far, m) for m in range(1, count)]

    scalar = pl.BlockSpec(memory_space=pltpu.SMEM)
    vector = pl.BlockSpec(memory_space=pltpu.VMEM)
    square_shape = (count, PANEL_WIDTH, BLOCK_WIDTH)
    inverse_shape = (PANEL_WIDTH, BLOCK_WIDTH)
    where = me.reshape(1).astype(jnp.int32)
    upper, inverse = pl.pallas_call(
        first_kernel,
        out_shape=(jax.ShapeDtypeStruct(square_shape, F32), jax.ShapeDtypeStruct(inverse_shape, F32)),
        in_specs=[scalar] + [vector] * (2 * count + 2),
        out_specs=(vector, vector),
        scratch_shapes=[pltpu.VMEM((span, span), F32)],
        name="first_panel",
    )(where, *diags, *diag_tiles, row_hot, col_hot)
    mine, send = pl.pallas_call(
        second_kernel,
        out_shape=(
            jax.ShapeDtypeStruct((BLOCK_WIDTH, 2 * PANEL_WIDTH), F32),
            jax.ShapeDtypeStruct((BLOCK_WIDTH, PANEL_WIDTH), BF16),
        ),
        in_specs=[scalar] + [vector] * (3 * count + 5),
        out_specs=(vector, vector),
        scratch_shapes=[
            pltpu.VMEM(square_shape, F32),
            pltpu.VMEM(square_shape, F32),
            pltpu.VMEM(inverse_shape, F32),
            pltpu.VMEM((span, span), F32),
        ],
        name="second_panel",
    )(where, *sides, *fars, *tiles, upper, inverse, row_hot, far_row_hot, far_col_hot)
    got = swap(send, count).astype(F32)
    theirs = jnp.concatenate([jnp.zeros_like(got), got], axis=1)
    return jnp.where(half == 0, mine, theirs)[None]


def on_device(front, child, index_map):
    cycle_size = lax.axis_size("blk")
    if COL_BLOCKS == 1 and cycle_size * BLOCK_WIDTH == 2 * PANEL_WIDTH and front.shape[0] == 1:
        return two_panels(front, child, index_map)
    return any_cycle(front, child, index_map)


def from_behind(shard, axis, by):
    count = lax.axis_size(axis)
    return lax.ppermute(shard, axis, [(i, (i + by) % count) for i in range(count)])


def column_numbers(cycle_size, my_index):
    local_ids = jnp.arange(COL_BLOCKS * BLOCK_WIDTH, dtype=jnp.int32)
    return (
        local_ids // BLOCK_WIDTH * cycle_size + my_index
    ) * BLOCK_WIDTH + local_ids % BLOCK_WIDTH


def row_numbers(cycle_size):
    stored = jnp.arange(cycle_size * COL_BLOCKS * BLOCK_WIDTH, dtype=jnp.int32)
    holder = stored // (COL_BLOCKS * BLOCK_WIDTH)
    within = stored // BLOCK_WIDTH % COL_BLOCKS
    return (within * cycle_size + holder) * BLOCK_WIDTH + stored % BLOCK_WIDTH


def cycle_rows(matrix, cycle_size):
    height = matrix.shape[0]
    return (
        matrix.reshape(height, COL_BLOCKS, cycle_size, BLOCK_WIDTH)
        .transpose(0, 2, 1, 3)
        .reshape(height, -1)
    )


def natural_rows(matrix, cycle_size):
    height = matrix.shape[0]
    return (
        matrix.reshape(height, cycle_size, COL_BLOCKS, BLOCK_WIDTH)
        .transpose(0, 2, 1, 3)
        .reshape(height, -1)
    )


def panel_rows(matrix, row_start, cycle_size):
    first_owner = row_start // BLOCK_WIDTH
    owner_count = PANEL_WIDTH // BLOCK_WIDTH
    height = matrix.shape[0]
    blocks = matrix.reshape(height, cycle_size, COL_BLOCKS, BLOCK_WIDTH)
    return blocks[:, first_owner : first_owner + owner_count, 0, :].reshape(height, PANEL_WIDTH)


def ownership(row_start, my_index):
    first_owner = row_start // BLOCK_WIDTH
    owner_count = PANEL_WIDTH // BLOCK_WIDTH
    is_owner = (my_index >= first_owner) & (my_index < first_owner + owner_count)
    column_start = jnp.clip(my_index - first_owner, 0, owner_count - 1) * BLOCK_WIDTH
    return (is_owner, column_start)


def collect(stacked, row_start, my_index):
    is_owner, column_start = ownership(row_start, my_index)
    padded = jnp.zeros((stacked.shape[0], PANEL_WIDTH, PANEL_WIDTH), jnp.float32)
    padded = lax.dynamic_update_slice(
        padded, jnp.where(is_owner, stacked, 0.0), (0, column_start, 0)
    )
    result = lax.psum(padded, "blk")
    return result


def own_rows(diag_factor, panel_part, row_start, columns):
    solved = lax.linalg.triangular_solve(
        diag_factor, panel_part, left_side=False, lower=True, transpose_a=True
    )
    offsets = columns - row_start
    diag_rows = jnp.take(diag_factor, jnp.clip(offsets, 0, PANEL_WIDTH - 1), axis=0)
    inside = (offsets >= 0) & (offsets < PANEL_WIDTH)
    before = offsets < 0
    return jnp.where(inside[:, None], diag_rows, jnp.where(before[:, None], 0.0, solved))


def make_refresh(working, lowered, owned_panels):

    def refresh(received, offset):
        updated = working - lax.dot_general(
            lowered, received, (((1,), (1,)), ((), ())), preferred_element_type=jnp.float32
        )
        leading = updated
        for is_owner, column_start in owned_panels:
            factor_column = (
                lax.dynamic_slice_in_dim(received, column_start, BLOCK_WIDTH, 1)
                .astype(jnp.float32)
                .T
            )
            leading = jnp.where(is_owner, factor_column, leading)
        return jnp.concatenate([leading, updated[BLOCK_WIDTH:]], axis=0)

    return refresh


def assemble(front, child, index_map, cycle_size, my_index):
    half_cycle = cycle_size // 2
    arrived_tiles = from_behind(child, "blk", half_cycle)
    full_order = 2 * index_map.shape[0]
    tile_places = (index_map % BLOCK_WIDTH).reshape(COL_BLOCKS, cycle_size, TILE_WIDTH)
    places = jnp.arange(BLOCK_WIDTH, dtype=jnp.int32)
    row_table = (tile_places[..., None] == places).astype(jnp.float32)
    shaped = arrived_tiles.reshape(COL_BLOCKS, TILE_WIDTH, COL_BLOCKS, cycle_size, TILE_WIDTH)
    spread = jnp.einsum("acbei,beiq->acbeq", shaped, row_table, precision=HIGHEST)
    spread = jnp.roll(spread, half_cycle, axis=3).reshape(COL_BLOCKS, TILE_WIDTH, full_order)
    source = (my_index - half_cycle) % cycle_size
    own_places = lax.dynamic_index_in_dim(tile_places, source, axis=1, keepdims=False)
    column_table = (own_places[..., None] == places).astype(jnp.float32)
    placed = jnp.einsum("kcq,kcn->kqn", column_table, spread, precision=HIGHEST)
    return front + placed


def any_cycle(front, child, index_map):
    cycle_size = lax.axis_size("blk")
    my_index = lax.axis_index("blk")
    local_width = COL_BLOCKS * BLOCK_WIDTH
    assembled = assemble(front, child, index_map, cycle_size, my_index).reshape(local_width, -1)
    working = cycle_rows(assembled, cycle_size)
    columns = column_numbers(cycle_size, my_index)
    for row_start in (0, PANEL_WIDTH):
        panel_part = panel_rows(working, row_start, cycle_size)
        diag_block = collect(panel_part[None, :BLOCK_WIDTH], row_start, my_index)[0]
        lowered = own_rows(jnp.linalg.cholesky(diag_block), panel_part, row_start, columns).astype(
            jnp.bfloat16
        )
        refresh = make_refresh(working, lowered, (ownership(row_start, my_index),))
        working = refresh(lax.all_gather(lowered, "blk", axis=0, tiled=True), jnp.int32(0))
    trailing = columns >= 2 * PANEL_WIDTH
    leading_rows = row_numbers(cycle_size) < 2 * PANEL_WIDTH
    working = jnp.where(trailing[:, None] & leading_rows[None, :], 0.0, working)
    return natural_rows(working, cycle_size).reshape(COL_BLOCKS, BLOCK_WIDTH, -1)


def solution(mesh):
    placed = (P("front", "blk", None), P("front", "blk", None), P("front"))
    return jax.shard_map(
        on_device, mesh=mesh, in_specs=placed, out_specs=P("front", "blk", None), check_vma=False
    )
```

```python
import jax
import jax.numpy as jnp
from jax import lax
from jax.experimental import pallas as pl
from jax.experimental.pallas import tpu as pltpu
from jax.sharding import PartitionSpec as P


PANEL_WIDTH = 512
BLOCK_WIDTH = 128
COL_BLOCKS = 1
TILE_WIDTH = 64


HIGHEST = lax.Precision.HIGHEST


F32 = jnp.float32
BF16 = jnp.bfloat16
LANES = 128
SUBS = 8
WIDTH = 2
GROUP = 4
KERNEL_BYTES = 16 * 1024 * 1024


def lane_copy(tile, lane):
    return jnp.broadcast_to(tile[:, lane:lane+1], tile.shape)


def row_copy(tile, row):
    return jnp.broadcast_to(tile[row:row+1, :], tile.shape)


def tree_sum(terms):
    while len(terms) > 1:
        terms = [a + b for a, b in zip(terms[::2], terms[1::2])] + ([terms[-1]] if len(terms) % 2 else [])
    return terms[0]


def halves(x):
    high = x.astype(BF16)
    return high, (x - high.astype(F32)).astype(BF16)


def product3(left, right):
    (lh, ll), (rh, rl) = left, right
    mm = lambda x, y: jnp.dot(x, y, preferred_element_type=F32)
    return mm(lh, rh) + (mm(lh, rl) + mm(ll, rh))


def eliminate(tiles, start_lane, zero):
    count = len(tiles)
    tiles = list(tiles)
    shape = (SUBS, LANES)
    lane = lax.broadcasted_iota(jnp.int32, shape, 1)
    sub = lax.broadcasted_iota(jnp.int32, shape, 0)
    at_row = [sub == k for k in range(SUBS)]
    uppers, inverses = [], []
    for head in range(0, count, WIDTH):
        own = range(WIDTH)
        span = WIDTH * SUBS
        first = start_lane + head * SUBS
        inside = (lane >= first) & (lane < first + span)
        cols = [[None] * span for _ in own]
        for m in range(span):
            for t in own:
                cols[t][m] = lane_copy(tiles[head + t], first + m) + zero
        later = {}
        for m in range(span):
            for i in range(head + WIDTH, count):
                later[i, m] = lane_copy(tiles[i], first + m)
        plain = [tiles[head + t] for t in own]
        joined = [
            jnp.where(inside, jnp.where(lane - (first + t * SUBS) == sub, 1.0, 0.0), plain[t]) for t in own
        ]
        upper = [jnp.zeros(shape, F32) for _ in own]
        inverse = [jnp.zeros(shape, F32) for _ in own]
        for k in range(span):
            at, r = divmod(k, SUBS)
            root = lax.rsqrt(row_copy(cols[at][k], r))
            inv = root * root
            weight = [jnp.where(at_row[r], -1.0, cols[t][k]) if t == at else cols[t][k] for t in own]
            for m in range(k + 1, span):
                pivot = row_copy(cols[at][m], r)
                for t in own:
                    kept = jnp.where(at_row[r], 0.0, cols[t][m]) if t == at else cols[t][m]
                    if m == k + 1:
                        cols[t][m] = kept - (weight[t] * pivot) * inv
                    else:
                        if t == 0:
                            scaled = pivot * inv
                        cols[t][m] = kept - weight[t] * scaled
            pivot = row_copy(plain[at], r)
            upper[at] = jnp.where(at_row[r], pivot * root, upper[at])
            scaled = pivot * inv
            for t in range(at, WIDTH):
                plain[t] = plain[t] - weight[t] * scaled
            pivot = row_copy(joined[at], r)
            inverse[at] = jnp.where(at_row[r], pivot * root, inverse[at])
            scaled = pivot * inv
            for t in own:
                kept = jnp.where(at_row[r], 0.0, joined[t]) if t == at else joined[t]
                joined[t] = kept - weight[t] * scaled
        for t in own:
            diag = first + t * SUBS + sub
            uppers.append(jnp.where(lane >= diag, upper[t], 0.0))
            inverses.append(jnp.where(lane <= diag, inverse[t], 0.0))
        rows = [row_copy(joined[k // SUBS], k % SUBS) for k in range(span)]
        for i in range(head + WIDTH, count):
            update = tree_sum([later[i, k] * rows[k] for k in range(span)])
            tiles[i] = jnp.where(inside, 0.0, tiles[i]) - update
    return uppers, inverses


def factor_tiles(tiles, zero):
    tiles = list(tiles)
    lane = lax.broadcasted_iota(jnp.int32, (SUBS, LANES), 1)
    uppers, inverses = [], []
    for g in range(0, len(tiles), GROUP):
        up, inv = eliminate(tiles[g:g+GROUP], g*SUBS, zero)
        uppers += up; inverses += inv
        done = (g + GROUP) * SUBS
        rest = len(tiles) - g - GROUP
        if rest:
            z = jnp.concatenate([jnp.where(lane < done, a, b) for a, b in zip(inv, up)], axis=0)
            left = z.T[done:, :]
            upd = product3(halves(left), halves(z))
            for t in range(rest):
                i = g + GROUP + t
                tiles[i] = jnp.where((lane >= g*SUBS) & (lane < done), 0.0, tiles[i]) - upd[8*t:8*t+8, :]
    return uppers, inverses


def block_rows(b):
    return pl.ds(pl.multiple_of(b * BLOCK_WIDTH, BLOCK_WIDTH), BLOCK_WIDTH)


def exact_parts(values):
    parts = []
    for _ in range(3):
        parts.append(values.astype(BF16))
        values = values - parts[-1].astype(F32)
    return parts


def place_columns(part, col_hot, q):
    pair = 2 * TILE_WIDTH
    return jnp.dot(
        part[:, q * pair : (q + 1) * pair], col_hot[q * pair : (q + 1) * pair, :], preferred_element_type=F32
    )


def lay_square(me, slabs, square):
    count = len(slabs)
    for m in range(count):
        owner = jnp.bitwise_xor(me, m)
        for step in range(count - 1):
            square[(owner + step) % count, block_rows(owner), :] = slabs[m][
                :, step * BLOCK_WIDTH : (step + 1) * BLOCK_WIDTH
            ]


def close_square(square):
    count = square.shape[0]
    square[count - 1, :BLOCK_WIDTH, :] = square[0, (count - 1) * BLOCK_WIDTH : count * BLOCK_WIDTH, :].T


def factor_panel(square, inverse, zero):
    count = square.shape[0]
    for b in range(count):
        base = b * BLOCK_WIDTH
        rows = slice(base, base + BLOCK_WIDTH)
        tiles = [square[b, base + SUBS * t : base + SUBS * (t + 1), :] for t in range(BLOCK_WIDTH // SUBS)]
        uppers, inverses = factor_tiles(tiles, zero)
        own_inverse = jnp.concatenate(inverses, axis=0)
        square[b, rows, :] = jnp.concatenate(uppers, axis=0)
        inverse[rows, :] = own_inverse
        scale = halves(own_inverse)
        lefts = {}
        for j in range(b + 1, count):
            value = product3(scale, halves(square[j, rows, :]))
            square[j, rows, :] = value
            right = halves(value)
            lefts[j] = halves(value.T)
            for i in range(b + 1, j + 1):
                square[j, i * BLOCK_WIDTH : (i + 1) * BLOCK_WIDTH, :] -= product3(lefts[i], right)


def spread_rows(kids, row_hot, col_hot, full):
    pair = 2 * TILE_WIDTH
    pairs = kids.shape[1] // pair
    parts = [
        jnp.dot(row_hot[...], part, preferred_element_type=F32).astype(BF16) for part in exact_parts(kids[...])
    ]
    for q in range(pairs):
        total = sum(place_columns(part, col_hot, (q + pairs // 2) % pairs) for part in parts)
        for which in range(2):
            full[2 * q + which] = total[:, which * BLOCK_WIDTH : (which + 1) * BLOCK_WIDTH]


def block_lanes(j):
    return slice(j * BLOCK_WIDTH, (j + 1) * BLOCK_WIDTH)


def rows_kernel(where, slab, kids, row_hot, col_hot, diag, side, full):
    count = PANEL_WIDTH // BLOCK_WIDTH
    me, half = where[0], where[1]
    spread_rows(kids, row_hot, col_hot, full)
    for j in range(2 * count):
        full[j] += slab[:, block_lanes(j)]
    for step in range(count - 1):
        diag[:, block_lanes(step)] = full[half * count + (me + step) % count]
    for j in range(count):
        side[:, block_lanes(j)] = full[(1 - half) * count + j]


def far_kernel(where, raw, kids, row_hot, col_hot, out, full):
    count = PANEL_WIDTH // BLOCK_WIDTH
    me, half = where[0], where[1]
    spread_rows(kids, row_hot, col_hot, full)
    for step in range(count - 1):
        out[:, block_lanes(step)] = raw[:, block_lanes(step)] + full[(1 - half) * count + (me + step) % count]


def first_kernel(where, *refs):
    count = PANEL_WIDTH // BLOCK_WIDTH
    slabs, (upper, inverse) = refs[:count], refs[count:]
    lay_square(where[0], slabs, upper)
    close_square(upper)
    factor_panel(upper, inverse, slabs[0][:SUBS, :LANES] * 0.0)


def second_kernel(where, *refs):
    count = PANEL_WIDTH // BLOCK_WIDTH
    sides, fars = refs[:count], refs[count : 2 * count]
    upper, inverse, mine, send, side, square, own_inverse = refs[2 * count :]
    me, half = where[0], where[1]
    for m in range(count):
        side[block_rows(jnp.bitwise_xor(me, m)), :] = sides[m][...]
    lay_square(me, fars, square)
    close_square(square)
    for b in range(count):
        rows = slice(b * BLOCK_WIDTH, (b + 1) * BLOCK_WIDTH)
        value = product3(halves(inverse[rows, :]), halves(side[rows, :]))
        side[rows, :] = value
        solved = halves(value)
        for i in range(b + 1, count):
            side[i * BLOCK_WIDTH : (i + 1) * BLOCK_WIDTH, :] -= product3(halves(upper[i, rows, :].T), solved)
    rounded = side[...].astype(BF16)
    for i in range(count):
        left = rounded[:, i * BLOCK_WIDTH : (i + 1) * BLOCK_WIDTH].T
        total = jnp.dot(left, rounded[:, i * BLOCK_WIDTH :], preferred_element_type=F32)
        for j in range(i, count):
            square[j, i * BLOCK_WIDTH : (i + 1) * BLOCK_WIDTH, :] -= total[
                :, (j - i) * BLOCK_WIDTH : (j - i + 1) * BLOCK_WIDTH
            ]
    factor_panel(square, own_inverse, sides[0][:SUBS, :LANES] * 0.0)
    rows = block_rows(me)
    for j in range(count):
        kept = (j >= me) & (half == 0)
        mine[:, block_lanes(j)] = jnp.where(kept, upper[j, rows, :], 0.0).astype(BF16).astype(F32)
        send[:, block_lanes(j)] = jnp.where(j >= me, square[j, rows, :], 0.0).astype(BF16)
    mine[:, PANEL_WIDTH:] = side[rows, :].astype(BF16).astype(F32)


def finish_kernel(where, mine, got, out, done):
    @pl.when(where[1] == 1)
    def _():
        mine[:, PANEL_WIDTH:] = got[...].astype(F32)

    copy = pltpu.make_async_copy(mine, out, done)
    copy.start()
    copy.wait()


def two_panels(front, child, index_map):
    cycle_size = lax.axis_size("blk")
    my_index = lax.axis_index("blk")
    count = PANEL_WIDTH // BLOCK_WIDTH
    me = my_index % count
    half = my_index // count

    def swap(shard, by):
        return lax.ppermute(shard, "blk", [(i, i ^ by) for i in range(cycle_size)])

    def share(shard):
        return [shard] + [swap(shard, m) for m in range(1, count)]

    def row_hot(block):
        own = lax.dynamic_slice_in_dim(places, block * TILE_WIDTH, TILE_WIDTH)
        return (jnp.arange(BLOCK_WIDTH, dtype=jnp.int32)[:, None] == own).astype(BF16)

    places = index_map % BLOCK_WIDTH
    tiles = jnp.arange(places.shape[0], dtype=jnp.int32) // TILE_WIDTH
    col_hot = ((places + tiles % 2 * BLOCK_WIDTH)[:, None] == jnp.arange(2 * BLOCK_WIDTH, dtype=jnp.int32)).astype(BF16)

    scalar = pl.BlockSpec(memory_space=pltpu.SMEM)
    vector = pl.BlockSpec(memory_space=pltpu.VMEM)
    where = jnp.stack([me, half]).astype(jnp.int32)
    square_shape = (count, PANEL_WIDTH, BLOCK_WIDTH)
    inverse_shape = (PANEL_WIDTH, BLOCK_WIDTH)
    diag_shape = (BLOCK_WIDTH, (count - 1) * BLOCK_WIDTH)
    side_shape = (BLOCK_WIDTH, PANEL_WIDTH)
    full = pltpu.VMEM((cycle_size, BLOCK_WIDTH, BLOCK_WIDTH), F32)

    grant = pltpu.CompilerParams(vmem_limit_bytes=KERNEL_BYTES)

    def near(array):
        return pltpu.with_memory_space_constraint(array, pltpu.VMEM)

    def local(kernel, outs, ins, scratch=()):
        return pl.pallas_call(
            kernel,
            out_shape=[pltpu.VMEM(*out) for out in outs],
            in_specs=[scalar] + [vector] * len(ins),
            out_specs=[vector] * len(outs),
            scratch_shapes=scratch,
            compiler_params=grant,
        )(where, *[near(array) for array in ins])

    slab, kids = front[0], child[0]
    arrived = swap(kids, count)
    raw = jnp.concatenate(
        [
            lax.dynamic_slice_in_dim(slab, (half * count + (me + step) % count) * BLOCK_WIDTH, BLOCK_WIDTH, 1)
            for step in range(count - 1)
        ],
        axis=1,
    )
    far = swap(raw, count)
    own_hot, far_hot = row_hot((my_index + count) % cycle_size), row_hot(my_index)
    diag, side = local(rows_kernel, [(diag_shape, F32), (side_shape, F32)], [slab, arrived, own_hot, col_hot], [full])
    diags = share(diag)
    sides = share(side)
    (far,) = local(far_kernel, [(diag_shape, F32)], [far, kids, far_hot, col_hot], [full])
    fars = share(far)
    upper, inverse = local(first_kernel, [(square_shape, F32), (inverse_shape, F32)], diags)
    mine, send = local(
        second_kernel,
        [((BLOCK_WIDTH, 2 * PANEL_WIDTH), F32), (side_shape, BF16)],
        [*sides, *fars, upper, inverse],
        [
            pltpu.VMEM((PANEL_WIDTH, PANEL_WIDTH), F32),
            pltpu.VMEM(square_shape, F32),
            pltpu.VMEM(inverse_shape, F32),
        ],
    )
    got = swap(send, count)
    result = pl.pallas_call(
        finish_kernel,
        out_shape=jax.ShapeDtypeStruct((BLOCK_WIDTH, 2 * PANEL_WIDTH), F32),
        in_specs=[scalar, vector, vector],
        out_specs=pl.BlockSpec(memory_space=pl.ANY),
        scratch_shapes=[pltpu.SemaphoreType.DMA],
        compiler_params=grant,
        name="finish",
    )(where, near(mine), near(got))
    return result[None]


def is_two_panels(cycle_size):
    return COL_BLOCKS == 1 and cycle_size * BLOCK_WIDTH == 2 * PANEL_WIDTH


def on_device(front, child, index_map):
    if is_two_panels(lax.axis_size("blk")):
        return two_panels(front, child, index_map)
    return any_cycle(front, child, index_map)


def from_behind(shard, axis, by):
    count = lax.axis_size(axis)
    return lax.ppermute(shard, axis, [(i, (i + by) % count) for i in range(count)])


def column_numbers(cycle_size, my_index):
    local_ids = jnp.arange(COL_BLOCKS * BLOCK_WIDTH, dtype=jnp.int32)
    return (
        local_ids // BLOCK_WIDTH * cycle_size + my_index
    ) * BLOCK_WIDTH + local_ids % BLOCK_WIDTH


def row_numbers(cycle_size):
    stored = jnp.arange(cycle_size * COL_BLOCKS * BLOCK_WIDTH, dtype=jnp.int32)
    holder = stored // (COL_BLOCKS * BLOCK_WIDTH)
    within = stored // BLOCK_WIDTH % COL_BLOCKS
    return (within * cycle_size + holder) * BLOCK_WIDTH + stored % BLOCK_WIDTH


def cycle_rows(matrix, cycle_size):
    height = matrix.shape[0]
    return (
        matrix.reshape(height, COL_BLOCKS, cycle_size, BLOCK_WIDTH)
        .transpose(0, 2, 1, 3)
        .reshape(height, -1)
    )


def natural_rows(matrix, cycle_size):
    height = matrix.shape[0]
    return (
        matrix.reshape(height, cycle_size, COL_BLOCKS, BLOCK_WIDTH)
        .transpose(0, 2, 1, 3)
        .reshape(height, -1)
    )


def panel_rows(matrix, row_start, cycle_size):
    first_owner = row_start // BLOCK_WIDTH
    owner_count = PANEL_WIDTH // BLOCK_WIDTH
    height = matrix.shape[0]
    blocks = matrix.reshape(height, cycle_size, COL_BLOCKS, BLOCK_WIDTH)
    return blocks[:, first_owner : first_owner + owner_count, 0, :].reshape(height, PANEL_WIDTH)


def ownership(row_start, my_index):
    first_owner = row_start // BLOCK_WIDTH
    owner_count = PANEL_WIDTH // BLOCK_WIDTH
    is_owner = (my_index >= first_owner) & (my_index < first_owner + owner_count)
    column_start = jnp.clip(my_index - first_owner, 0, owner_count - 1) * BLOCK_WIDTH
    return (is_owner, column_start)


def collect(stacked, row_start, my_index):
    is_owner, column_start = ownership(row_start, my_index)
    padded = jnp.zeros((stacked.shape[0], PANEL_WIDTH, PANEL_WIDTH), jnp.float32)
    padded = lax.dynamic_update_slice(
        padded, jnp.where(is_owner, stacked, 0.0), (0, column_start, 0)
    )
    result = lax.psum(padded, "blk")
    return result


def own_rows(diag_factor, panel_part, row_start, columns):
    solved = lax.linalg.triangular_solve(
        diag_factor, panel_part, left_side=False, lower=True, transpose_a=True
    )
    offsets = columns - row_start
    diag_rows = jnp.take(diag_factor, jnp.clip(offsets, 0, PANEL_WIDTH - 1), axis=0)
    inside = (offsets >= 0) & (offsets < PANEL_WIDTH)
    before = offsets < 0
    return jnp.where(inside[:, None], diag_rows, jnp.where(before[:, None], 0.0, solved))


def make_refresh(working, lowered, owned_panels):

    def refresh(received, offset):
        updated = working - lax.dot_general(
            lowered, received, (((1,), (1,)), ((), ())), preferred_element_type=jnp.float32
        )
        leading = updated
        for is_owner, column_start in owned_panels:
            factor_column = (
                lax.dynamic_slice_in_dim(received, column_start, BLOCK_WIDTH, 1)
                .astype(jnp.float32)
                .T
            )
            leading = jnp.where(is_owner, factor_column, leading)
        return jnp.concatenate([leading, updated[BLOCK_WIDTH:]], axis=0)

    return refresh


def assemble(front, child, index_map, cycle_size, my_index):
    half_cycle = cycle_size // 2
    arrived_tiles = from_behind(child, "blk", half_cycle)
    full_order = 2 * index_map.shape[0]
    tile_places = (index_map % BLOCK_WIDTH).reshape(COL_BLOCKS, cycle_size, TILE_WIDTH)
    places = jnp.arange(BLOCK_WIDTH, dtype=jnp.int32)
    row_table = (tile_places[..., None] == places).astype(jnp.float32)
    shaped = arrived_tiles.reshape(COL_BLOCKS, TILE_WIDTH, COL_BLOCKS, cycle_size, TILE_WIDTH)
    spread = jnp.einsum("acbei,beiq->acbeq", shaped, row_table, precision=HIGHEST)
    spread = jnp.roll(spread, half_cycle, axis=3).reshape(COL_BLOCKS, TILE_WIDTH, full_order)
    source = (my_index - half_cycle) % cycle_size
    own_places = lax.dynamic_index_in_dim(tile_places, source, axis=1, keepdims=False)
    column_table = (own_places[..., None] == places).astype(jnp.float32)
    placed = jnp.einsum("kcq,kcn->kqn", column_table, spread, precision=HIGHEST)
    return front + placed


def any_cycle(front, child, index_map):
    cycle_size = lax.axis_size("blk")
    my_index = lax.axis_index("blk")
    local_width = COL_BLOCKS * BLOCK_WIDTH
    assembled = assemble(front, child, index_map, cycle_size, my_index).reshape(local_width, -1)
    working = cycle_rows(assembled, cycle_size)
    columns = column_numbers(cycle_size, my_index)
    for row_start in (0, PANEL_WIDTH):
        panel_part = panel_rows(working, row_start, cycle_size)
        diag_block = collect(panel_part[None, :BLOCK_WIDTH], row_start, my_index)[0]
        lowered = own_rows(jnp.linalg.cholesky(diag_block), panel_part, row_start, columns).astype(
            jnp.bfloat16
        )
        refresh = make_refresh(working, lowered, (ownership(row_start, my_index),))
        working = refresh(lax.all_gather(lowered, "blk", axis=0, tiled=True), jnp.int32(0))
    trailing = columns >= 2 * PANEL_WIDTH
    leading_rows = row_numbers(cycle_size) < 2 * PANEL_WIDTH
    working = jnp.where(trailing[:, None] & leading_rows[None, :], 0.0, working)
    return natural_rows(working, cycle_size).reshape(COL_BLOCKS, BLOCK_WIDTH, -1)


def solution(mesh):
    placed = (P("front", "blk", None), P("front", "blk", None), P("front"))
    return jax.shard_map(
        on_device, mesh=mesh, in_specs=placed, out_specs=P("front", "blk", None), check_vma=False
    )
```

```python
import jax
import jax.numpy as jnp
from jax import lax
from jax.experimental import pallas as pl
from jax.experimental.pallas import tpu as pltpu
from jax.sharding import PartitionSpec as P


PANEL_WIDTH = 512
BLOCK_WIDTH = 128
COL_BLOCKS = 1
TILE_WIDTH = 64


HIGHEST = lax.Precision.HIGHEST


F32 = jnp.float32
BF16 = jnp.bfloat16
LANES = 128
SUBS = 8
WIDTH = 2
GROUP = 16
KERNEL_BYTES = 16 * 1024 * 1024


def lane_copy(tile, lane):
    return jnp.broadcast_to(tile[:, lane:lane+1], tile.shape)


def row_copy(tile, row):
    return jnp.broadcast_to(tile[row:row+1, :], tile.shape)


def tree_sum(terms):
    while len(terms) > 1:
        terms = [a + b for a, b in zip(terms[::2], terms[1::2])] + ([terms[-1]] if len(terms) % 2 else [])
    return terms[0]


def halves(x):
    high = x.astype(BF16)
    return high, (x - high.astype(F32)).astype(BF16)


def product3(left, right):
    (lh, ll), (rh, rl) = left, right
    mm = lambda x, y: jnp.dot(x, y, preferred_element_type=F32)
    return mm(lh, rh) + (mm(lh, rl) + mm(ll, rh))


def eliminate(tiles, start_lane, zero):
    count = len(tiles)
    tiles = list(tiles)
    shape = (SUBS, LANES)
    lane = lax.broadcasted_iota(jnp.int32, shape, 1)
    sub = lax.broadcasted_iota(jnp.int32, shape, 0)
    at_row = [sub == k for k in range(SUBS)]
    unit = [jnp.where(at, 1.0, 0.0) for at in at_row]
    results = []
    own = range(WIDTH)
    span = WIDTH * SUBS
    for head in range(0, count, WIDTH):
        first = start_lane + head * SUBS
        inside = (lane >= first) & (lane < first + span)
        cols = [[None] * span for _ in own]
        for m in range(span):
            for t in own:
                cols[t][m] = lane_copy(tiles[head + t], first + m) + (zero if t == 0 else 0.0)
        later = {}
        for m in range(span):
            for i in range(head + WIDTH, count):
                later[i, m] = lane_copy(tiles[i], first + m)
        joined = [
            jnp.where(inside, jnp.where(lane - (first + t * SUBS) == sub, 1.0, 0.0), tiles[head + t]) for t in own
        ]
        result = [jnp.zeros(shape, F32) for _ in own]
        for k in range(span):
            at, r = divmod(k, SUBS)
            root = lax.rsqrt(row_copy(cols[at][k], r))
            inv = root * root
            weight = [cols[t][k] - unit[r] if t == at else cols[t][k] for t in own]
            for m in range(k + 1, span):
                pivot = row_copy(cols[at][m], r)
                if m == k + 1:
                    for t in own:
                        cols[t][m] = cols[t][m] - (weight[t] * pivot) * inv
                else:
                    pivot = pivot * inv
                    for t in own:
                        cols[t][m] = cols[t][m] - weight[t] * pivot
            pivot = row_copy(joined[at], r)
            result[at] = jnp.where(at_row[r], pivot * root, result[at])
            pivot = pivot * inv
            for t in own:
                joined[t] = joined[t] - weight[t] * pivot
        results += result
        rows = [row_copy(joined[k // SUBS], k % SUBS) for k in range(span)]
        for i in range(head + WIDTH, count):
            update = tree_sum([later[i, k] * rows[k] for k in range(span)])
            tiles[i] = jnp.where(inside, 0.0, tiles[i]) - update
    return results


def inverse_tiles(tiles, zero):
    tiles = list(tiles)
    lane = lax.broadcasted_iota(jnp.int32, (SUBS, LANES), 1)
    sub = lax.broadcasted_iota(jnp.int32, (SUBS, LANES), 0)
    inverses = []
    for g in range(0, len(tiles), GROUP):
        results = eliminate(tiles[g : g + GROUP], g * SUBS, zero)
        kept = [jnp.where(lane <= (g + t) * SUBS + sub, result, 0.0) for t, result in enumerate(results)]
        inverses += kept
        done = (g + GROUP) * SUBS
        if done < BLOCK_WIDTH:
            scaled = jnp.concatenate(
                [jnp.where(lane < done, low, result) for low, result in zip(kept, results)], axis=0
            )
            update = product3(halves(scaled.T[done:, :]), halves(scaled))
            group_lanes = (lane >= g * SUBS) & (lane < done)
            for t in range(g + GROUP, len(tiles)):
                at = t * SUBS - done
                tiles[t] = jnp.where(group_lanes, 0.0, tiles[t]) - update[at : at + SUBS, :]
    return inverses


def block_rows(b):
    return pl.ds(pl.multiple_of(b * BLOCK_WIDTH, BLOCK_WIDTH), BLOCK_WIDTH)


def block_lanes(j):
    return slice(j * BLOCK_WIDTH, (j + 1) * BLOCK_WIDTH)


def exact_parts(values):
    parts = []
    for _ in range(3):
        parts.append(values.astype(BF16))
        values = values - parts[-1].astype(F32)
    return parts


def place_columns(part, col_hot, q):
    pair = 2 * TILE_WIDTH
    return jnp.dot(
        part[:, q * pair : (q + 1) * pair], col_hot[q * pair : (q + 1) * pair, :], preferred_element_type=F32
    )


def lay_square(me, slabs, square):
    count = len(slabs)
    for m in range(count):
        owner = jnp.bitwise_xor(me, m)
        for step in range(slabs[m].shape[1] // BLOCK_WIDTH):
            square[(owner + step) % count, block_rows(owner), :] = slabs[m][:, block_lanes(step)]
    square[count - 1, :BLOCK_WIDTH, :] = square[0, (count - 1) * BLOCK_WIDTH : count * BLOCK_WIDTH, :].T
    across = count // 2

    @pl.when(me >= across)
    def _():
        for b in range(across):
            square[b + across, block_lanes(b), :] = square[b, block_lanes(b + across), :].T


def factor_panel(square, inverse, zero):
    count = square.shape[0]
    above = lax.broadcasted_iota(jnp.int32, (BLOCK_WIDTH, BLOCK_WIDTH), 0) <= lax.broadcasted_iota(
        jnp.int32, (BLOCK_WIDTH, BLOCK_WIDTH), 1
    )
    for b in range(count):
        base = b * BLOCK_WIDTH
        rows = slice(base, base + BLOCK_WIDTH)
        tiles = [square[b, base + SUBS * t : base + SUBS * (t + 1), :] for t in range(BLOCK_WIDTH // SUBS)]
        own_inverse = jnp.concatenate(inverse_tiles(tiles, zero), axis=0)
        inverse[rows, :] = own_inverse
        scale = halves(own_inverse)
        lefts = {}
        for j in range(b + 1, count):
            value = product3(scale, halves(square[j, rows, :]))
            square[j, rows, :] = value
            right = halves(value)
            lefts[j] = halves(value.T)
            for i in range(b + 1, j + 1):
                square[j, i * BLOCK_WIDTH : (i + 1) * BLOCK_WIDTH, :] -= product3(lefts[i], right)
        square[b, rows, :] = jnp.where(above, product3(scale, halves(square[b, rows, :])), 0.0)


def spread_rows(kids, row_hot, col_hot, full):
    pair = 2 * TILE_WIDTH
    pairs = kids.shape[1] // pair
    parts = [
        jnp.dot(row_hot[...], part, preferred_element_type=F32).astype(BF16) for part in exact_parts(kids[...])
    ]
    for q in range(pairs):
        total = sum(place_columns(part, col_hot, (q + pairs // 2) % pairs) for part in parts)
        for which in range(2):
            full[2 * q + which] = total[:, which * BLOCK_WIDTH : (which + 1) * BLOCK_WIDTH]


def rows_kernel(where, slab, kids, row_hot, col_hot, diag, wide_diag, side, full):
    count = PANEL_WIDTH // BLOCK_WIDTH
    me, half = where[0], where[1]
    spread_rows(kids, row_hot, col_hot, full)
    for j in range(2 * count):
        full[j] += slab[:, block_lanes(j)]
    for step in range(count - 1):
        wide_diag[:, block_lanes(step)] = full[half * count + (me + step) % count]
    diag[...] = wide_diag[:, : diag.shape[1]]
    for j in range(count):
        side[:, block_lanes(j)] = full[(1 - half) * count + j]


def far_kernel(where, raw, kids, row_hot, col_hot, out, wide_out, full):
    count = PANEL_WIDTH // BLOCK_WIDTH
    me, half = where[0], where[1]
    spread_rows(kids, row_hot, col_hot, full)
    for step in range(count - 1):
        wide_out[:, block_lanes(step)] = raw[:, block_lanes(step)] + full[(1 - half) * count + (me + step) % count]
    out[...] = wide_out[:, : out.shape[1]]


def first_kernel(where, *refs):
    count = PANEL_WIDTH // BLOCK_WIDTH
    slabs, (upper, inverse) = refs[:count], refs[count:]
    lay_square(where[0], slabs, upper)
    factor_panel(upper, inverse, slabs[0][:SUBS, :LANES] * 0.0)


def second_kernel(where, *refs):
    count = PANEL_WIDTH // BLOCK_WIDTH
    sides, fars = refs[:count], refs[count : 2 * count]
    upper, inverse, mine, send, side, square, own_inverse = refs[2 * count :]
    me, half = where[0], where[1]
    for m in range(count):
        side[block_rows(jnp.bitwise_xor(me, m)), :] = sides[m][...]
    lay_square(me, fars, square)
    for b in range(count):
        rows = slice(b * BLOCK_WIDTH, (b + 1) * BLOCK_WIDTH)
        value = product3(halves(inverse[rows, :]), halves(side[rows, :]))
        side[rows, :] = value
        solved = halves(value)
        for i in range(b + 1, count):
            side[i * BLOCK_WIDTH : (i + 1) * BLOCK_WIDTH, :] -= product3(halves(upper[i, rows, :].T), solved)
    rounded = side[...].astype(BF16)
    for i in range(count):
        left = rounded[:, i * BLOCK_WIDTH : (i + 1) * BLOCK_WIDTH].T
        total = jnp.dot(left, rounded[:, i * BLOCK_WIDTH :], preferred_element_type=F32)
        for j in range(i, count):
            square[j, i * BLOCK_WIDTH : (i + 1) * BLOCK_WIDTH, :] -= total[
                :, (j - i) * BLOCK_WIDTH : (j - i + 1) * BLOCK_WIDTH
            ]
    factor_panel(square, own_inverse, sides[0][:SUBS, :LANES] * 0.0)
    rows = block_rows(me)
    for j in range(count):
        kept = (j >= me) & (half == 0)
        mine[:, block_lanes(j)] = jnp.where(kept, upper[j, rows, :], 0.0).astype(BF16).astype(F32)
        send[:, block_lanes(j)] = jnp.where(j >= me, square[j, rows, :], 0.0).astype(BF16)
    mine[:, PANEL_WIDTH:] = side[rows, :].astype(BF16).astype(F32)


def finish_kernel(where, mine, got, out, done):
    @pl.when(where[1] == 1)
    def _():
        mine[:, PANEL_WIDTH:] = got[...].astype(F32)

    copy = pltpu.make_async_copy(mine, out, done)
    copy.start()
    copy.wait()


def two_panels(front, child, index_map):
    cycle_size = lax.axis_size("blk")
    my_index = lax.axis_index("blk")
    count = PANEL_WIDTH // BLOCK_WIDTH
    me = my_index % count
    half = my_index // count

    def swap(shard, by):
        return lax.ppermute(shard, "blk", [(i, i ^ by) for i in range(cycle_size)])

    def share(shard, wide):
        return [wide] + [swap(wide if m == 1 else shard, m) for m in range(1, count)]

    def row_hot(block):
        own = lax.dynamic_slice_in_dim(places, block * TILE_WIDTH, TILE_WIDTH)
        return (jnp.arange(BLOCK_WIDTH, dtype=jnp.int32)[:, None] == own).astype(BF16)

    places = index_map % BLOCK_WIDTH
    tiles = jnp.arange(places.shape[0], dtype=jnp.int32) // TILE_WIDTH
    col_hot = ((places + tiles % 2 * BLOCK_WIDTH)[:, None] == jnp.arange(2 * BLOCK_WIDTH, dtype=jnp.int32)).astype(BF16)

    scalar = pl.BlockSpec(memory_space=pltpu.SMEM)
    vector = pl.BlockSpec(memory_space=pltpu.VMEM)
    where = jnp.stack([me, half]).astype(jnp.int32)
    square_shape = (count, PANEL_WIDTH, BLOCK_WIDTH)
    inverse_shape = (PANEL_WIDTH, BLOCK_WIDTH)
    diag_shape = (BLOCK_WIDTH, (count - 2) * BLOCK_WIDTH)
    wide_shape = (BLOCK_WIDTH, (count - 1) * BLOCK_WIDTH)
    side_shape = (BLOCK_WIDTH, PANEL_WIDTH)
    full = pltpu.VMEM((cycle_size, BLOCK_WIDTH, BLOCK_WIDTH), F32)

    grant = pltpu.CompilerParams(vmem_limit_bytes=KERNEL_BYTES)

    def near(array):
        return pltpu.with_memory_space_constraint(array, pltpu.VMEM)

    def local(kernel, outs, ins, scratch=()):
        return pl.pallas_call(
            kernel,
            out_shape=[pltpu.VMEM(*out) for out in outs],
            in_specs=[scalar] + [vector] * len(ins),
            out_specs=[vector] * len(outs),
            scratch_shapes=scratch,
            compiler_params=grant,
        )(where, *[near(array) for array in ins])

    slab, kids = front[0], child[0]
    arrived = swap(kids, count)
    raw = jnp.concatenate(
        [
            lax.dynamic_slice_in_dim(slab, (half * count + (me + step) % count) * BLOCK_WIDTH, BLOCK_WIDTH, 1)
            for step in range(count - 1)
        ],
        axis=1,
    )
    far = swap(raw, count)
    own_hot, far_hot = row_hot((my_index + count) % cycle_size), row_hot(my_index)
    diag, wide_diag, side = local(
        rows_kernel,
        [(diag_shape, F32), (wide_shape, F32), (side_shape, F32)],
        [slab, arrived, own_hot, col_hot],
        [full],
    )
    diags = share(diag, wide_diag)
    sides = share(side, side)
    far, wide_far = local(far_kernel, [(diag_shape, F32), (wide_shape, F32)], [far, kids, far_hot, col_hot], [full])
    fars = share(far, wide_far)
    upper, inverse = local(first_kernel, [(square_shape, F32), (inverse_shape, F32)], diags)
    mine, send = local(
        second_kernel,
        [((BLOCK_WIDTH, 2 * PANEL_WIDTH), F32), (side_shape, BF16)],
        [*sides, *fars, upper, inverse],
        [
            pltpu.VMEM((PANEL_WIDTH, PANEL_WIDTH), F32),
            pltpu.VMEM(square_shape, F32),
            pltpu.VMEM(inverse_shape, F32),
        ],
    )
    got = swap(send, count)
    result = pl.pallas_call(
        finish_kernel,
        out_shape=jax.ShapeDtypeStruct((BLOCK_WIDTH, 2 * PANEL_WIDTH), F32),
        in_specs=[scalar, vector, vector],
        out_specs=pl.BlockSpec(memory_space=pl.ANY),
        scratch_shapes=[pltpu.SemaphoreType.DMA],
        compiler_params=grant,
        name="finish",
    )(where, near(mine), near(got))
    return result[None]


def is_two_panels(cycle_size):
    return COL_BLOCKS == 1 and cycle_size * BLOCK_WIDTH == 2 * PANEL_WIDTH


def on_device(front, child, index_map):
    if is_two_panels(lax.axis_size("blk")):
        return two_panels(front, child, index_map)
    return any_cycle(front, child, index_map)


def from_behind(shard, axis, by):
    count = lax.axis_size(axis)
    return lax.ppermute(shard, axis, [(i, (i + by) % count) for i in range(count)])


def column_numbers(cycle_size, my_index):
    local_ids = jnp.arange(COL_BLOCKS * BLOCK_WIDTH, dtype=jnp.int32)
    return (
        local_ids // BLOCK_WIDTH * cycle_size + my_index
    ) * BLOCK_WIDTH + local_ids % BLOCK_WIDTH


def row_numbers(cycle_size):
    stored = jnp.arange(cycle_size * COL_BLOCKS * BLOCK_WIDTH, dtype=jnp.int32)
    holder = stored // (COL_BLOCKS * BLOCK_WIDTH)
    within = stored // BLOCK_WIDTH % COL_BLOCKS
    return (within * cycle_size + holder) * BLOCK_WIDTH + stored % BLOCK_WIDTH


def cycle_rows(matrix, cycle_size):
    height = matrix.shape[0]
    return (
        matrix.reshape(height, COL_BLOCKS, cycle_size, BLOCK_WIDTH)
        .transpose(0, 2, 1, 3)
        .reshape(height, -1)
    )


def natural_rows(matrix, cycle_size):
    height = matrix.shape[0]
    return (
        matrix.reshape(height, cycle_size, COL_BLOCKS, BLOCK_WIDTH)
        .transpose(0, 2, 1, 3)
        .reshape(height, -1)
    )


def panel_rows(matrix, row_start, cycle_size):
    first_owner = row_start // BLOCK_WIDTH
    owner_count = PANEL_WIDTH // BLOCK_WIDTH
    height = matrix.shape[0]
    blocks = matrix.reshape(height, cycle_size, COL_BLOCKS, BLOCK_WIDTH)
    return blocks[:, first_owner : first_owner + owner_count, 0, :].reshape(height, PANEL_WIDTH)


def ownership(row_start, my_index):
    first_owner = row_start // BLOCK_WIDTH
    owner_count = PANEL_WIDTH // BLOCK_WIDTH
    is_owner = (my_index >= first_owner) & (my_index < first_owner + owner_count)
    column_start = jnp.clip(my_index - first_owner, 0, owner_count - 1) * BLOCK_WIDTH
    return (is_owner, column_start)


def collect(stacked, row_start, my_index):
    is_owner, column_start = ownership(row_start, my_index)
    padded = jnp.zeros((stacked.shape[0], PANEL_WIDTH, PANEL_WIDTH), jnp.float32)
    padded = lax.dynamic_update_slice(
        padded, jnp.where(is_owner, stacked, 0.0), (0, column_start, 0)
    )
    result = lax.psum(padded, "blk")
    return result


def own_rows(diag_factor, panel_part, row_start, columns):
    solved = lax.linalg.triangular_solve(
        diag_factor, panel_part, left_side=False, lower=True, transpose_a=True
    )
    offsets = columns - row_start
    diag_rows = jnp.take(diag_factor, jnp.clip(offsets, 0, PANEL_WIDTH - 1), axis=0)
    inside = (offsets >= 0) & (offsets < PANEL_WIDTH)
    before = offsets < 0
    return jnp.where(inside[:, None], diag_rows, jnp.where(before[:, None], 0.0, solved))


def make_refresh(working, lowered, owned_panels):

    def refresh(received, offset):
        updated = working - lax.dot_general(
            lowered, received, (((1,), (1,)), ((), ())), preferred_element_type=jnp.float32
        )
        leading = updated
        for is_owner, column_start in owned_panels:
            factor_column = (
                lax.dynamic_slice_in_dim(received, column_start, BLOCK_WIDTH, 1)
                .astype(jnp.float32)
                .T
            )
            leading = jnp.where(is_owner, factor_column, leading)
        return jnp.concatenate([leading, updated[BLOCK_WIDTH:]], axis=0)

    return refresh


def assemble(front, child, index_map, cycle_size, my_index):
    half_cycle = cycle_size // 2
    arrived_tiles = from_behind(child, "blk", half_cycle)
    full_order = 2 * index_map.shape[0]
    tile_places = (index_map % BLOCK_WIDTH).reshape(COL_BLOCKS, cycle_size, TILE_WIDTH)
    places = jnp.arange(BLOCK_WIDTH, dtype=jnp.int32)
    row_table = (tile_places[..., None] == places).astype(jnp.float32)
    shaped = arrived_tiles.reshape(COL_BLOCKS, TILE_WIDTH, COL_BLOCKS, cycle_size, TILE_WIDTH)
    spread = jnp.einsum("acbei,beiq->acbeq", shaped, row_table, precision=HIGHEST)
    spread = jnp.roll(spread, half_cycle, axis=3).reshape(COL_BLOCKS, TILE_WIDTH, full_order)
    source = (my_index - half_cycle) % cycle_size
    own_places = lax.dynamic_index_in_dim(tile_places, source, axis=1, keepdims=False)
    column_table = (own_places[..., None] == places).astype(jnp.float32)
    placed = jnp.einsum("kcq,kcn->kqn", column_table, spread, precision=HIGHEST)
    return front + placed


def any_cycle(front, child, index_map):
    cycle_size = lax.axis_size("blk")
    my_index = lax.axis_index("blk")
    local_width = COL_BLOCKS * BLOCK_WIDTH
    assembled = assemble(front, child, index_map, cycle_size, my_index).reshape(local_width, -1)
    working = cycle_rows(assembled, cycle_size)
    columns = column_numbers(cycle_size, my_index)
    for row_start in (0, PANEL_WIDTH):
        panel_part = panel_rows(working, row_start, cycle_size)
        diag_block = collect(panel_part[None, :BLOCK_WIDTH], row_start, my_index)[0]
        lowered = own_rows(jnp.linalg.cholesky(diag_block), panel_part, row_start, columns).astype(
            jnp.bfloat16
        )
        refresh = make_refresh(working, lowered, (ownership(row_start, my_index),))
        working = refresh(lax.all_gather(lowered, "blk", axis=0, tiled=True), jnp.int32(0))
    trailing = columns >= 2 * PANEL_WIDTH
    leading_rows = row_numbers(cycle_size) < 2 * PANEL_WIDTH
    working = jnp.where(trailing[:, None] & leading_rows[None, :], 0.0, working)
    return natural_rows(working, cycle_size).reshape(COL_BLOCKS, BLOCK_WIDTH, -1)


def solution(mesh):
    placed = (P("front", "blk", None), P("front", "blk", None), P("front"))
    return jax.shard_map(
        on_device, mesh=mesh, in_specs=placed, out_specs=P("front", "blk", None), check_vma=False
    )
```

```python
import jax
import jax.numpy as jnp
from jax import lax
from jax.experimental import pallas as pl
from jax.experimental.pallas import tpu as pltpu
from jax.sharding import PartitionSpec as P


PANEL_WIDTH = 512
BLOCK_WIDTH = 128
COL_BLOCKS = 1
TILE_WIDTH = 64


HIGHEST = lax.Precision.HIGHEST


F32 = jnp.float32
BF16 = jnp.bfloat16
LANES = 128
SUBS = 8
WIDTH = 2
GROUP = 16
KERNEL_BYTES = 16 * 1024 * 1024


def lane_copy(tile, lane):
    return jnp.broadcast_to(tile[:, lane:lane+1], tile.shape)


def row_copy(tile, row):
    return jnp.broadcast_to(tile[row:row+1, :], tile.shape)


def tree_sum(terms):
    while len(terms) > 1:
        terms = [a + b for a, b in zip(terms[::2], terms[1::2])] + ([terms[-1]] if len(terms) % 2 else [])
    return terms[0]


def halves(x):
    high = x.astype(BF16)
    return high, (x - high.astype(F32)).astype(BF16)


def product3(left, right):
    (lh, ll), (rh, rl) = left, right
    mm = lambda x, y: jnp.dot(x, y, preferred_element_type=F32)
    return mm(lh, rh) + (mm(lh, rl) + mm(ll, rh))


def eliminate(tiles, start_lane, zero):
    count = len(tiles)
    tiles = list(tiles)
    shape = (SUBS, LANES)
    lane = lax.broadcasted_iota(jnp.int32, shape, 1)
    sub = lax.broadcasted_iota(jnp.int32, shape, 0)
    at_row = [sub == k for k in range(SUBS)]
    unit = [jnp.where(at, 1.0, 0.0) for at in at_row]
    results = []
    own = range(WIDTH)
    span = WIDTH * SUBS
    for head in range(0, count, WIDTH):
        first = start_lane + head * SUBS
        inside = (lane >= first) & (lane < first + span)
        cols = [[None] * span for _ in own]
        for m in range(span):
            for t in own:
                cols[t][m] = lane_copy(tiles[head + t], first + m) + (zero if t == 0 else 0.0)
        later = {}
        for m in range(span):
            for i in range(head + WIDTH, count):
                later[i, m] = lane_copy(tiles[i], first + m)
        joined = [
            jnp.where(inside, jnp.where(lane - (first + t * SUBS) == sub, 1.0, 0.0), tiles[head + t]) for t in own
        ]
        result = [jnp.zeros(shape, F32) for _ in own]
        for k in range(span):
            at, r = divmod(k, SUBS)
            root = lax.rsqrt(row_copy(cols[at][k], r))
            inv = root * root
            weight = [cols[t][k] - unit[r] if t == at else cols[t][k] for t in own]
            for m in range(k + 1, span):
                pivot = row_copy(cols[at][m], r)
                if m == k + 1:
                    for t in own:
                        cols[t][m] = cols[t][m] - (weight[t] * pivot) * inv
                else:
                    pivot = pivot * inv
                    for t in own:
                        cols[t][m] = cols[t][m] - weight[t] * pivot
            pivot = row_copy(joined[at], r)
            result[at] = jnp.where(at_row[r], pivot * root, result[at])
            pivot = pivot * inv
            for t in own:
                joined[t] = joined[t] - weight[t] * pivot
        results += result
        rows = [row_copy(joined[k // SUBS], k % SUBS) for k in range(span)]
        for i in range(head + WIDTH, count):
            update = tree_sum([later[i, k] * rows[k] for k in range(span)])
            tiles[i] = jnp.where(inside, 0.0, tiles[i]) - update
    return results


def inverse_tiles(tiles, zero):
    tiles = list(tiles)
    lane = lax.broadcasted_iota(jnp.int32, (SUBS, LANES), 1)
    sub = lax.broadcasted_iota(jnp.int32, (SUBS, LANES), 0)
    inverses = []
    for g in range(0, len(tiles), GROUP):
        results = eliminate(tiles[g : g + GROUP], g * SUBS, zero)
        kept = [jnp.where(lane <= (g + t) * SUBS + sub, result, 0.0) for t, result in enumerate(results)]
        inverses += kept
        done = (g + GROUP) * SUBS
        if done < BLOCK_WIDTH:
            scaled = jnp.concatenate(
                [jnp.where(lane < done, low, result) for low, result in zip(kept, results)], axis=0
            )
            update = product3(halves(scaled.T[done:, :]), halves(scaled))
            group_lanes = (lane >= g * SUBS) & (lane < done)
            for t in range(g + GROUP, len(tiles)):
                at = t * SUBS - done
                tiles[t] = jnp.where(group_lanes, 0.0, tiles[t]) - update[at : at + SUBS, :]
    return inverses


def block_rows(b):
    return pl.ds(pl.multiple_of(b * BLOCK_WIDTH, BLOCK_WIDTH), BLOCK_WIDTH)


def block_lanes(j):
    return slice(j * BLOCK_WIDTH, (j + 1) * BLOCK_WIDTH)


def exact_parts(values):
    parts = []
    for _ in range(3):
        parts.append(values.astype(BF16))
        values = values - parts[-1].astype(F32)
    return parts


def place_columns(part, col_hot, q):
    pair = 2 * TILE_WIDTH
    return jnp.dot(
        part[:, q * pair : (q + 1) * pair], col_hot[q * pair : (q + 1) * pair, :], preferred_element_type=F32
    )


def lay_square(me, slabs, square):
    count = len(slabs)
    for m in range(count):
        owner = jnp.bitwise_xor(me, m)
        for step in range(slabs[m].shape[1] // BLOCK_WIDTH):
            square[(owner + step) % count, block_rows(owner), :] = slabs[m][:, block_lanes(step)]
    square[count - 1, :BLOCK_WIDTH, :] = square[0, (count - 1) * BLOCK_WIDTH : count * BLOCK_WIDTH, :].T
    across = count // 2

    @pl.when(me >= across)
    def _():
        for b in range(across):
            square[b + across, block_lanes(b), :] = square[b, block_lanes(b + across), :].T


def factor_panel(square, inverse, zero):
    count = square.shape[0]
    above = lax.broadcasted_iota(jnp.int32, (BLOCK_WIDTH, BLOCK_WIDTH), 0) <= lax.broadcasted_iota(
        jnp.int32, (BLOCK_WIDTH, BLOCK_WIDTH), 1
    )
    for b in range(count):
        base = b * BLOCK_WIDTH
        rows = slice(base, base + BLOCK_WIDTH)
        tiles = [square[b, base + SUBS * t : base + SUBS * (t + 1), :] for t in range(BLOCK_WIDTH // SUBS)]
        own_inverse = jnp.concatenate(inverse_tiles(tiles, zero), axis=0)
        inverse[rows, :] = own_inverse
        scale = halves(own_inverse)
        lefts = {}
        for j in range(b + 1, count):
            value = product3(scale, halves(square[j, rows, :]))
            square[j, rows, :] = value
            right = halves(value)
            lefts[j] = halves(value.T)
            for i in range(b + 1, j + 1):
                square[j, i * BLOCK_WIDTH : (i + 1) * BLOCK_WIDTH, :] -= product3(lefts[i], right)
        square[b, rows, :] = jnp.where(above, product3(scale, halves(square[b, rows, :])), 0.0)


def spread_rows(kids, row_hot, col_hot, full):
    pair = 2 * TILE_WIDTH
    pairs = kids.shape[1] // pair
    parts = [
        jnp.dot(row_hot[...], part, preferred_element_type=F32).astype(BF16) for part in exact_parts(kids[...])
    ]
    for q in range(pairs):
        total = sum(place_columns(part, col_hot, (q + pairs // 2) % pairs) for part in parts)
        for which in range(2):
            full[2 * q + which] = total[:, which * BLOCK_WIDTH : (which + 1) * BLOCK_WIDTH]


def rows_kernel(where, slab, kids, row_hot, col_hot, diag, wide_diag, side, full):
    count = PANEL_WIDTH // BLOCK_WIDTH
    me, half = where[0], where[1]
    spread_rows(kids, row_hot, col_hot, full)
    for j in range(2 * count):
        full[j] += slab[:, block_lanes(j)]
    for step in range(count - 1):
        wide_diag[:, block_lanes(step)] = full[half * count + (me + step) % count]
    diag[...] = wide_diag[:, : diag.shape[1]]
    for j in range(count):
        side[:, block_lanes(j)] = full[(1 - half) * count + j]


def far_kernel(where, raw, kids, row_hot, col_hot, out, wide_out, full):
    count = PANEL_WIDTH // BLOCK_WIDTH
    me, half = where[0], where[1]
    spread_rows(kids, row_hot, col_hot, full)
    for step in range(count - 1):
        wide_out[:, block_lanes(step)] = raw[:, block_lanes(step)] + full[(1 - half) * count + (me + step) % count]
    out[...] = wide_out[:, : out.shape[1]]


def first_kernel(where, *refs):
    count = PANEL_WIDTH // BLOCK_WIDTH
    slabs, (upper, inverse) = refs[:count], refs[count:]
    lay_square(where[0], slabs, upper)
    factor_panel(upper, inverse, slabs[0][:SUBS, :LANES] * 0.0)


def second_kernel(where, *refs):
    count = PANEL_WIDTH // BLOCK_WIDTH
    sides, fars = refs[:count], refs[count : 2 * count]
    upper, inverse, out, keep, send, side, square, own_inverse, left_rows, done = refs[2 * count :]
    me, half = where[0], where[1]
    for m in range(count):
        side[block_rows(jnp.bitwise_xor(me, m)), :] = sides[m][...]
    lay_square(me, fars, square)
    for b in range(count):
        rows = slice(b * BLOCK_WIDTH, (b + 1) * BLOCK_WIDTH)
        value = product3(halves(inverse[rows, :]), halves(side[rows, :]))
        side[rows, :] = value
        solved = halves(value)
        for i in range(b + 1, count):
            side[i * BLOCK_WIDTH : (i + 1) * BLOCK_WIDTH, :] -= product3(halves(upper[i, rows, :].T), solved)
    rows = block_rows(me)
    for j in range(count):
        kept = (j >= me) & (half == 0)
        left_rows[:, block_lanes(j)] = jnp.where(kept, upper[j, rows, :], 0.0).astype(BF16).astype(F32)
    copy = pltpu.make_async_copy(left_rows, out.at[:, :PANEL_WIDTH], done)
    copy.start()
    keep[...] = side[rows, :].astype(BF16).astype(F32)
    rounded = side[...].astype(BF16)
    for i in range(count):
        left = rounded[:, i * BLOCK_WIDTH : (i + 1) * BLOCK_WIDTH].T
        total = jnp.dot(left, rounded[:, i * BLOCK_WIDTH :], preferred_element_type=F32)
        for j in range(i, count):
            square[j, i * BLOCK_WIDTH : (i + 1) * BLOCK_WIDTH, :] -= total[
                :, (j - i) * BLOCK_WIDTH : (j - i + 1) * BLOCK_WIDTH
            ]
    factor_panel(square, own_inverse, sides[0][:SUBS, :LANES] * 0.0)
    for j in range(count):
        send[:, block_lanes(j)] = jnp.where(j >= me, square[j, rows, :], 0.0).astype(BF16)
    copy.wait()


def finish_kernel(where, begun, keep, got, out, wide, done):
    del begun
    wide[...] = jnp.where(where[1] == 1, got[...].astype(F32), keep[...])
    copy = pltpu.make_async_copy(wide, out.at[:, PANEL_WIDTH:], done)
    copy.start()
    copy.wait()


def two_panels(front, child, index_map):
    cycle_size = lax.axis_size("blk")
    my_index = lax.axis_index("blk")
    count = PANEL_WIDTH // BLOCK_WIDTH
    me = my_index % count
    half = my_index // count

    def swap(shard, by):
        return lax.ppermute(shard, "blk", [(i, i ^ by) for i in range(cycle_size)])

    def share(shard, wide):
        return [wide] + [swap(wide if m == 1 else shard, m) for m in range(1, count)]

    def row_hot(block):
        own = lax.dynamic_slice_in_dim(places, block * TILE_WIDTH, TILE_WIDTH)
        return (jnp.arange(BLOCK_WIDTH, dtype=jnp.int32)[:, None] == own).astype(BF16)

    places = index_map % BLOCK_WIDTH
    tiles = jnp.arange(places.shape[0], dtype=jnp.int32) // TILE_WIDTH
    col_hot = ((places + tiles % 2 * BLOCK_WIDTH)[:, None] == jnp.arange(2 * BLOCK_WIDTH, dtype=jnp.int32)).astype(BF16)

    scalar = pl.BlockSpec(memory_space=pltpu.SMEM)
    vector = pl.BlockSpec(memory_space=pltpu.VMEM)
    anywhere = pl.BlockSpec(memory_space=pl.ANY)
    where = jnp.stack([me, half]).astype(jnp.int32)
    square_shape = (count, PANEL_WIDTH, BLOCK_WIDTH)
    inverse_shape = (PANEL_WIDTH, BLOCK_WIDTH)
    diag_shape = (BLOCK_WIDTH, (count - 2) * BLOCK_WIDTH)
    wide_shape = (BLOCK_WIDTH, (count - 1) * BLOCK_WIDTH)
    side_shape = (BLOCK_WIDTH, PANEL_WIDTH)
    full = pltpu.VMEM((cycle_size, BLOCK_WIDTH, BLOCK_WIDTH), F32)

    grant = pltpu.CompilerParams(vmem_limit_bytes=KERNEL_BYTES)

    def near(array):
        return pltpu.with_memory_space_constraint(array, pltpu.VMEM)

    def local(kernel, outs, ins, scratch=()):
        return pl.pallas_call(
            kernel,
            out_shape=[out if isinstance(out, jax.ShapeDtypeStruct) else pltpu.VMEM(*out) for out in outs],
            in_specs=[scalar] + [vector] * len(ins),
            out_specs=[anywhere if isinstance(out, jax.ShapeDtypeStruct) else vector for out in outs],
            scratch_shapes=scratch,
            compiler_params=grant,
        )(where, *[near(array) for array in ins])

    slab, kids = front[0], child[0]
    arrived = swap(kids, count)
    raw = jnp.concatenate(
        [
            lax.dynamic_slice_in_dim(slab, (half * count + (me + step) % count) * BLOCK_WIDTH, BLOCK_WIDTH, 1)
            for step in range(count - 1)
        ],
        axis=1,
    )
    far = swap(raw, count)
    own_hot, far_hot = row_hot((my_index + count) % cycle_size), row_hot(my_index)
    diag, wide_diag, side = local(
        rows_kernel,
        [(diag_shape, F32), (wide_shape, F32), (side_shape, F32)],
        [slab, arrived, own_hot, col_hot],
        [full],
    )
    diags = share(diag, wide_diag)
    sides = share(side, side)
    far, wide_far = local(far_kernel, [(diag_shape, F32), (wide_shape, F32)], [far, kids, far_hot, col_hot], [full])
    fars = share(far, wide_far)
    upper, inverse = local(first_kernel, [(square_shape, F32), (inverse_shape, F32)], diags)
    begun, keep, send = local(
        second_kernel,
        [jax.ShapeDtypeStruct((BLOCK_WIDTH, 2 * PANEL_WIDTH), F32), (side_shape, F32), (side_shape, BF16)],
        [*sides, *fars, upper, inverse],
        [
            pltpu.VMEM((PANEL_WIDTH, PANEL_WIDTH), F32),
            pltpu.VMEM(square_shape, F32),
            pltpu.VMEM(inverse_shape, F32),
            pltpu.VMEM(side_shape, F32),
            pltpu.SemaphoreType.DMA,
        ],
    )
    got = swap(send, count)
    result = pl.pallas_call(
        finish_kernel,
        out_shape=jax.ShapeDtypeStruct((BLOCK_WIDTH, 2 * PANEL_WIDTH), F32),
        in_specs=[scalar, anywhere, vector, vector],
        out_specs=anywhere,
        input_output_aliases={1: 0},
        scratch_shapes=[pltpu.VMEM(side_shape, F32), pltpu.SemaphoreType.DMA],
        compiler_params=grant,
        name="finish",
    )(where, begun, near(keep), near(got))
    return result[None]


def is_two_panels(cycle_size):
    return COL_BLOCKS == 1 and cycle_size * BLOCK_WIDTH == 2 * PANEL_WIDTH


def on_device(front, child, index_map):
    if is_two_panels(lax.axis_size("blk")):
        return two_panels(front, child, index_map)
    return any_cycle(front, child, index_map)


def from_behind(shard, axis, by):
    count = lax.axis_size(axis)
    return lax.ppermute(shard, axis, [(i, (i + by) % count) for i in range(count)])


def column_numbers(cycle_size, my_index):
    local_ids = jnp.arange(COL_BLOCKS * BLOCK_WIDTH, dtype=jnp.int32)
    return (
        local_ids // BLOCK_WIDTH * cycle_size + my_index
    ) * BLOCK_WIDTH + local_ids % BLOCK_WIDTH


def row_numbers(cycle_size):
    stored = jnp.arange(cycle_size * COL_BLOCKS * BLOCK_WIDTH, dtype=jnp.int32)
    holder = stored // (COL_BLOCKS * BLOCK_WIDTH)
    within = stored // BLOCK_WIDTH % COL_BLOCKS
    return (within * cycle_size + holder) * BLOCK_WIDTH + stored % BLOCK_WIDTH


def cycle_rows(matrix, cycle_size):
    height = matrix.shape[0]
    return (
        matrix.reshape(height, COL_BLOCKS, cycle_size, BLOCK_WIDTH)
        .transpose(0, 2, 1, 3)
        .reshape(height, -1)
    )


def natural_rows(matrix, cycle_size):
    height = matrix.shape[0]
    return (
        matrix.reshape(height, cycle_size, COL_BLOCKS, BLOCK_WIDTH)
        .transpose(0, 2, 1, 3)
        .reshape(height, -1)
    )


def panel_rows(matrix, row_start, cycle_size):
    first_owner = row_start // BLOCK_WIDTH
    owner_count = PANEL_WIDTH // BLOCK_WIDTH
    height = matrix.shape[0]
    blocks = matrix.reshape(height, cycle_size, COL_BLOCKS, BLOCK_WIDTH)
    return blocks[:, first_owner : first_owner + owner_count, 0, :].reshape(height, PANEL_WIDTH)


def ownership(row_start, my_index):
    first_owner = row_start // BLOCK_WIDTH
    owner_count = PANEL_WIDTH // BLOCK_WIDTH
    is_owner = (my_index >= first_owner) & (my_index < first_owner + owner_count)
    column_start = jnp.clip(my_index - first_owner, 0, owner_count - 1) * BLOCK_WIDTH
    return (is_owner, column_start)


def collect(stacked, row_start, my_index):
    is_owner, column_start = ownership(row_start, my_index)
    padded = jnp.zeros((stacked.shape[0], PANEL_WIDTH, PANEL_WIDTH), jnp.float32)
    padded = lax.dynamic_update_slice(
        padded, jnp.where(is_owner, stacked, 0.0), (0, column_start, 0)
    )
    result = lax.psum(padded, "blk")
    return result


def own_rows(diag_factor, panel_part, row_start, columns):
    solved = lax.linalg.triangular_solve(
        diag_factor, panel_part, left_side=False, lower=True, transpose_a=True
    )
    offsets = columns - row_start
    diag_rows = jnp.take(diag_factor, jnp.clip(offsets, 0, PANEL_WIDTH - 1), axis=0)
    inside = (offsets >= 0) & (offsets < PANEL_WIDTH)
    before = offsets < 0
    return jnp.where(inside[:, None], diag_rows, jnp.where(before[:, None], 0.0, solved))


def make_refresh(working, lowered, owned_panels):

    def refresh(received, offset):
        updated = working - lax.dot_general(
            lowered, received, (((1,), (1,)), ((), ())), preferred_element_type=jnp.float32
        )
        leading = updated
        for is_owner, column_start in owned_panels:
            factor_column = (
                lax.dynamic_slice_in_dim(received, column_start, BLOCK_WIDTH, 1)
                .astype(jnp.float32)
                .T
            )
            leading = jnp.where(is_owner, factor_column, leading)
        return jnp.concatenate([leading, updated[BLOCK_WIDTH:]], axis=0)

    return refresh


def assemble(front, child, index_map, cycle_size, my_index):
    half_cycle = cycle_size // 2
    arrived_tiles = from_behind(child, "blk", half_cycle)
    full_order = 2 * index_map.shape[0]
    tile_places = (index_map % BLOCK_WIDTH).reshape(COL_BLOCKS, cycle_size, TILE_WIDTH)
    places = jnp.arange(BLOCK_WIDTH, dtype=jnp.int32)
    row_table = (tile_places[..., None] == places).astype(jnp.float32)
    shaped = arrived_tiles.reshape(COL_BLOCKS, TILE_WIDTH, COL_BLOCKS, cycle_size, TILE_WIDTH)
    spread = jnp.einsum("acbei,beiq->acbeq", shaped, row_table, precision=HIGHEST)
    spread = jnp.roll(spread, half_cycle, axis=3).reshape(COL_BLOCKS, TILE_WIDTH, full_order)
    source = (my_index - half_cycle) % cycle_size
    own_places = lax.dynamic_index_in_dim(tile_places, source, axis=1, keepdims=False)
    column_table = (own_places[..., None] == places).astype(jnp.float32)
    placed = jnp.einsum("kcq,kcn->kqn", column_table, spread, precision=HIGHEST)
    return front + placed


def any_cycle(front, child, index_map):
    cycle_size = lax.axis_size("blk")
    my_index = lax.axis_index("blk")
    local_width = COL_BLOCKS * BLOCK_WIDTH
    assembled = assemble(front, child, index_map, cycle_size, my_index).reshape(local_width, -1)
    working = cycle_rows(assembled, cycle_size)
    columns = column_numbers(cycle_size, my_index)
    for row_start in (0, PANEL_WIDTH):
        panel_part = panel_rows(working, row_start, cycle_size)
        diag_block = collect(panel_part[None, :BLOCK_WIDTH], row_start, my_index)[0]
        lowered = own_rows(jnp.linalg.cholesky(diag_block), panel_part, row_start, columns).astype(
            jnp.bfloat16
        )
        refresh = make_refresh(working, lowered, (ownership(row_start, my_index),))
        working = refresh(lax.all_gather(lowered, "blk", axis=0, tiled=True), jnp.int32(0))
    trailing = columns >= 2 * PANEL_WIDTH
    leading_rows = row_numbers(cycle_size) < 2 * PANEL_WIDTH
    working = jnp.where(trailing[:, None] & leading_rows[None, :], 0.0, working)
    return natural_rows(working, cycle_size).reshape(COL_BLOCKS, BLOCK_WIDTH, -1)


def solution(mesh):
    placed = (P("front", "blk", None), P("front", "blk", None), P("front"))
    return jax.shard_map(
        on_device, mesh=mesh, in_specs=placed, out_specs=P("front", "blk", None), check_vma=False
    )
```
